32 devices in a mesh: ctx: 4 (over y, x), tp: 8 (over z, core).
Axes of the slice: x: 2, y: 2, z: 4, core: 2. Of those that a mesh axis runs over, the one named last changes fastest.
Arguments:
- tokens: bfloat16 [2048, 4096], P(('ctx', 'tp')), may hold values from -16 to 16
- upstream: bfloat16 [2048, 4096], P('ctx', 'tp'), may hold values from -6 to 6
- w_query: bfloat16 [4096, 4096], P('ctx', 'tp')
- w_keyval: bfloat16 [4096, 2048], P('ctx', 'tp')
- positions: int32 [2048], replicated, may hold values from 0 to 2047, as said below
- documents: int32 [2048], replicated, may hold values from 0 to 3, never falling along the last dimension, each value on 1 to 1024 neighbouring positions
Outputs:
- token_grad: bfloat16 [2048, 4096], P(('ctx', 'tp'))
- query_grad: float32 [4096, 4096], P('ctx', 'tp')
- keyval_grad: float32 [4096, 2048], P('ctx', 'tp')
The draws below stay inside these ranges and needn't reach their ends.
Inputs may be any that keep to these rules, and one draw needn't show every extreme that they name: Each stored run of 512 tokens holds consecutive increasing positions; the two runs of the tokens of one context rank are the blocks k and 7 - k of the sequence for some k; all runs together hold every position once.
All inputs are finite; a program needn't handle non-finite values.
Results may differ from the reference program's by a relative error of at most 0.02.
The reference program's roundings to bfloat16 on the way count: a program that leaves them out, or rounds other values in their place, can miss the bound.
Values may be sent and summed in bfloat16 or wider, within the bound.
No kernel may reach another device: no remote copies, remote signals or barrier semaphores. Data moves between devices by JAX's collectives and lax.ppermute only.
A program may use at most 128 MiB of HBM per device.

```python
import math
import jax
import jax.numpy as jnp
import numpy as np
from jax import lax

MODEL_DIMENSION = 4096
QUERY_HEADS = 32
KEY_VALUE_HEADS = 8
HEAD_DIMENSION = 128
TOK_CTX = 512
DOCS = 4
SEQUENCE_TOKENS = 2048
BLOCK = 256
BLOCKS = 8
N_CTX = 4


def query_weight_matrix(key):
    rotary_base = jax.random.normal(jax.random.fold_in(key, 11), (MODEL_DIMENSION, QUERY_HEADS * HEAD_DIMENSION), jnp.float32)
    return jnp.clip(rotary_base, -6.0, 6.0) * MODEL_DIMENSION ** (-0.5)


def draw_tokens(key, part):
    rotary_base = jax.random.normal(jax.random.fold_in(key, 21), (SEQUENCE_TOKENS, MODEL_DIMENSION), jnp.float32)
    return jnp.clip(rotary_base, -16.0, 16.0).astype(jnp.bfloat16)


def draw_w_query(key, part):
    return query_weight_matrix(key).astype(jnp.bfloat16)


def draw_w_keyval(key, part):
    rotary_base = jax.random.normal(jax.random.fold_in(key, 12), (MODEL_DIMENSION, KEY_VALUE_HEADS, 2, HEAD_DIMENSION), jnp.float32)
    rotary_base = jnp.clip(rotary_base, -6.0, 6.0) * MODEL_DIMENSION ** (-0.5)
    return rotary_base.reshape(MODEL_DIMENSION, 2 * KEY_VALUE_HEADS * HEAD_DIMENSION).astype(jnp.bfloat16)


def draw_positions(key, part):
    pair_count = BLOCKS // 2
    pairs = jax.random.permutation(jax.random.fold_in(key, 31), pair_count).astype(jnp.int32)
    flips = jax.random.randint(jax.random.fold_in(key, 32), (pair_count,), 0, 2).astype(jnp.int32)
    leading = jnp.where(flips == 0, pairs, BLOCKS - 1 - pairs)
    trailing = BLOCKS - 1 - leading
    order = jnp.stack([leading, trailing], axis=1).reshape(BLOCKS)
    offsets = jnp.arange(BLOCK, dtype=jnp.int32)
    return (order[:, None] * BLOCK + offsets[None, :]).reshape(BLOCKS * BLOCK).astype(jnp.int32)


def with_spikes(values, own_key, source, target, shards_of, factor):
    def block_of(position):
        return (jnp.arange(values.shape[position]) // (values.shape[position] // shards_of)).reshape((-1,) + (1,) * (values.ndim - 1 - position))

    first = jax.random.permutation(own_key, shards_of)[block_of(target)]
    other_side = (block_of(target) + shards_of // 2) % shards_of
    return jnp.where((block_of(source) == first) | (block_of(source) == other_side), factor * values, values)


def levels(own_key, dims, cuts, smallest, high):
    gain = 1.0
    for axis_at, shards_of in cuts:
        heights = jax.random.uniform(jax.random.fold_in(jax.random.fold_in(own_key, 6), axis_at), (shards_of,), jnp.float32, smallest / len(cuts), high / len(cuts))
        gain = gain * jnp.repeat(jnp.exp(heights), dims[axis_at] // shards_of).reshape((-1,) + (1,) * (len(dims) - 1 - axis_at))
    return gain


def split_up(amount, total, limit, slope):
    portions = [(1 << 20) // math.isqrt(grade ** slope) + 1 for grade in range(2, amount + 1)]
    spare, holding = total - limit - (amount - 1), [1] * (amount - 1)
    while spare > 0:
        candidates = [i for i in range(amount - 1) if holding[i] < limit]
        pool, left = sum([portions[i] for i in candidates]), spare
        for i in candidates:
            more = min(limit - holding[i], max(1, left * portions[i] // pool), spare)
            holding[i] = holding[i] + more
            spare = spare - more
    return np.array([limit] + holding)


def uneven_parts(key, number_of, total, limit, skew):
    if number_of == 2:
        one = jax.random.randint(key, (), max(1, total - limit), min(limit, total - 1) + 1)
        return jnp.stack([one, total - one])
    sizes = jnp.asarray(split_up(number_of, total, limit, skew), jnp.int32)
    couples = (number_of - 1) // 2
    donor, sink = sizes[1:1 + 2 * couples:2], sizes[2:2 + 2 * couples:2]
    slack = jnp.minimum(donor - 1, limit - sink)
    shifted = jax.random.randint(jax.random.fold_in(key, 1), (couples,), 0, 1 << 20) % (slack + 1)
    sizes = sizes.at[1:1 + 2 * couples:2].set(donor - shifted).at[2:2 + 2 * couples:2].set(sink + shifted)
    return sizes[jax.random.permutation(jax.random.fold_in(key, 2), number_of)]


def bell_draw_with(stream_key, extent, spread, most, pieces, heavy, held_as=jnp.bfloat16):
    entries = spread * jax.random.normal(stream_key, extent, jnp.float32)
    if pieces:
        entries = entries * levels(stream_key, extent, pieces, -0.22, 0.18)
    return jnp.clip(with_spikes(entries, jax.random.fold_in(stream_key, 3), *heavy), -most, most).astype(held_as)


def setup_inputs(seed: int = 0) -> dict:
    splits = jax.random.split(jax.random.key(seed), 7)
    tokens = draw_tokens(jax.random.fold_in(splits[6], 71), 0)
    upstream = bell_draw_with(splits[1], (SEQUENCE_TOKENS, QUERY_HEADS * HEAD_DIMENSION), 1.0, 6.0, ((0, 4), (1, 8)), (1, 0, 8, 2.0))
    w_query = draw_w_query(jax.random.fold_in(splits[6], 71), 0)
    w_keyval = draw_w_keyval(jax.random.fold_in(splits[6], 71), 0)
    positions = draw_positions(jax.random.fold_in(splits[6], 71), 0)
    documents = jnp.searchsorted(jnp.cumsum(uneven_parts(splits[5], DOCS, SEQUENCE_TOKENS, SEQUENCE_TOKENS // 2, 2)), jnp.arange(SEQUENCE_TOKENS), side="right").astype(jnp.int32)
    return {"tokens": tokens, "upstream": upstream, "w_query": w_query, "w_keyval": w_keyval, "positions": positions, "documents": documents}


rope_base = 500000.0


def rotation_tables(positions):
    half_width = HEAD_DIMENSION // 2
    frequency = rope_base ** (-(jnp.arange(half_width, dtype=jnp.float32) * 2.0 / HEAD_DIMENSION))
    angles = positions.astype(jnp.float32)[:, None] * frequency[None, :]
    cosine = jnp.concatenate([jnp.cos(angles), jnp.cos(angles)], axis=1)
    sine = jnp.concatenate([jnp.sin(angles), jnp.sin(angles)], axis=1)
    return cosine, sine


def rotate(values, cosine, sine):
    half_width = values.shape[-1] // 2
    turned = jnp.concatenate([-values[..., half_width:], values[..., :half_width]], axis=-1)
    return values * cosine[:, None, :] + turned * sine[:, None, :]


def rotate_back(gradient, cosine, sine):
    half_width = gradient.shape[-1] // 2
    scaled = gradient * sine[:, None, :]
    turned = jnp.concatenate([scaled[..., half_width:], -scaled[..., :half_width]], axis=-1)
    return gradient * cosine[:, None, :] + turned


def reference(tokens, upstream, w_query, w_keyval, positions, documents):
    f32 = jnp.float32
    scaling = HEAD_DIMENSION ** -0.5
    query_raw = jnp.dot(tokens, w_query, preferred_element_type=f32)
    key_value_rows = jnp.dot(tokens, w_keyval, preferred_element_type=f32).astype(jnp.bfloat16)
    cosine, sine = rotation_tables(positions)
    query_rows = rotate(query_raw.reshape(SEQUENCE_TOKENS, QUERY_HEADS, HEAD_DIMENSION), cosine, sine).astype(jnp.bfloat16)
    key_value_quad = key_value_rows.reshape(SEQUENCE_TOKENS, KEY_VALUE_HEADS, 2, HEAD_DIMENSION)
    key = rotate(key_value_quad[:, :, 0].astype(f32), cosine, sine).astype(jnp.bfloat16)
    value = key_value_quad[:, :, 1]
    doc_of = jnp.take(documents, positions)
    visible = (positions[None, :] <= positions[:, None]) & (doc_of[None, :] == doc_of[:, None])
    group_width = QUERY_HEADS // KEY_VALUE_HEADS
    query_head_groups = query_rows.reshape(SEQUENCE_TOKENS, KEY_VALUE_HEADS, group_width, HEAD_DIMENSION).transpose(1, 0, 2, 3)
    gradient_groups = upstream.reshape(SEQUENCE_TOKENS, KEY_VALUE_HEADS, group_width, HEAD_DIMENSION).transpose(1, 0, 2, 3)
    key_groups = key.transpose(1, 0, 2)
    value_groups = value.transpose(1, 0, 2)

    def one_group(inputs):
        query_g, grad_g, key_g, value_g = inputs
        query_f = query_g.astype(f32)
        grad_f = grad_g.astype(f32)
        key_f = key_g.astype(f32)
        value_f = value_g.astype(f32)
        scores = jnp.einsum('qhd,kd->hqk', query_f, key_f) * scaling
        scores = jnp.where(visible[None], scores, -1e30)
        row_peak = jnp.max(scores, axis=-1, keepdims=True)
        exponent = jnp.exp(scores - row_peak)
        probs = exponent / jnp.sum(exponent, axis=-1, keepdims=True)
        probs_half = probs.astype(jnp.bfloat16).astype(f32)
        output = jnp.einsum('hqk,kd->qhd', probs_half, value_f)
        deltas = jnp.sum(grad_f * output, axis=-1)
        prob_grad = jnp.einsum('qhd,kd->hqk', grad_f, value_f)
        score_grad = (probs * (prob_grad - deltas.T[:, :, None])).astype(jnp.bfloat16).astype(f32)
        dquery = jnp.einsum('hqk,kd->qhd', score_grad, key_f) * scaling
        dkey = jnp.einsum('hqk,qhd->kd', score_grad, query_f) * scaling
        dvalue = jnp.einsum('hqk,qhd->kd', probs_half, grad_f)
        return dquery, dkey, dvalue

    dquery, dkey, dvalue = lax.map(one_group, (query_head_groups, gradient_groups, key_groups, value_groups))
    dquery = dquery.transpose(1, 0, 2, 3).reshape(SEQUENCE_TOKENS, QUERY_HEADS, HEAD_DIMENSION)
    query_back = rotate_back(dquery, cosine, sine).astype(jnp.bfloat16).reshape(SEQUENCE_TOKENS, QUERY_HEADS * HEAD_DIMENSION)
    key_backward = rotate_back(dkey.transpose(1, 0, 2), cosine, sine).astype(jnp.bfloat16)
    value_backward = dvalue.transpose(1, 0, 2).astype(jnp.bfloat16)
    key_value_backward = jnp.stack([key_backward, value_backward], axis=2).reshape(SEQUENCE_TOKENS, 2 * KEY_VALUE_HEADS * HEAD_DIMENSION)
    token_grad = jnp.dot(query_back, w_query.T, preferred_element_type=f32)
    token_grad = token_grad + jnp.dot(key_value_backward, w_keyval.T, preferred_element_type=f32)
    row_grads = jnp.concatenate([query_back, key_value_backward], axis=1)
    token_blocks = tokens.reshape(N_CTX, TOK_CTX, MODEL_DIMENSION)
    grad_blocks = row_grads.reshape(N_CTX, TOK_CTX, row_grads.shape[1])

    def accumulate(running, inputs):
        token_block, grad_block = inputs
        term = jnp.dot(token_block.T, grad_block, preferred_element_type=f32)
        term = lax.optimization_barrier(term.astype(jnp.bfloat16)).astype(f32)
        return running + term, None

    start_value = jnp.zeros((MODEL_DIMENSION, row_grads.shape[1]), f32)
    weight_grad, _ = lax.scan(accumulate, start_value, (token_blocks, grad_blocks))
    return token_grad.astype(jnp.bfloat16), weight_grad[:, :QUERY_HEADS * HEAD_DIMENSION], weight_grad[:, QUERY_HEADS * HEAD_DIMENSION:]
```

```python
import functools

import jax
import jax.numpy as jnp
from jax import lax
from jax.experimental import pallas as pl
from jax.experimental.pallas import tpu as pltpu
from jax.sharding import PartitionSpec as P

KEY_VALUE_HEADS = 8
HEAD = 128
ROPE_BASE = 500000.0


f32 = jnp.float32
bf16 = jnp.bfloat16


def swap(block, axis, mask):
    count = lax.axis_size(axis)
    return lax.ppermute(block, axis, [(i, i ^ mask) for i in range(count)])


def hop(block, step, first, last):
    return lax.ppermute(
        block, "tp", [(2 * z + c, 2 * (z + step) + c) for z in range(first, last + 1) for c in (0, 1)]
    )


def gather_ctx(block, bits):
    held = {0: block}
    for bit in bits:
        for j in list(held):
            held[j | bit] = swap(held[j], "ctx", bit)
    return held


def scatter_ctx(terms, bits):
    terms = dict(terms)
    for bit in bits:
        for j in sorted((j for j in terms if j & bit), reverse=True):
            got = swap(terms.pop(j).astype(bf16), "ctx", bit)
            terms[j ^ bit] = terms[j ^ bit].astype(bf16).astype(f32) + got.astype(f32)
    return terms[0]


def gather_line(block, pairs, z):
    right, left = {0: block}, {0: block}
    for s in range(1, pairs):
        right[s] = hop(right[s - 1], 1, s - 1, pairs - 2)
        left[s] = hop(left[s - 1], -1, 1, pairs - s)
    stack = jnp.zeros((pairs,) + block.shape, block.dtype)
    stack = lax.dynamic_update_index_in_dim(stack, block, z, 0)
    for s in range(1, pairs):
        come = jnp.where(z >= s, right[s], left[pairs - s])
        stack = lax.dynamic_update_index_in_dim(stack, come, (z - s) % pairs, 0)
    return stack


def scatter_line(stack, pairs, z):
    def pick(at):
        return lax.dynamic_index_in_dim(stack, at % pairs, 0, keepdims=False)

    total = pick(z)
    right, left = None, None
    for s in range(1, pairs):
        to_right, to_left = pick(z - s), pick(z + s)
        if right is not None:
            to_right = to_right + right.astype(f32)
            to_left = to_left + left.astype(f32)
        right = hop(to_right.astype(bf16), 1, 0, s - 1)
        left = hop(to_left.astype(bf16), -1, pairs - s, pairs - 1)
    return total + right.astype(f32) + left.astype(f32)


def nt(a, b):
    return lax.dot_general(a, b, (((1,), (1,)), ((), ())), preferred_element_type=f32)


def nn(a, b):
    return lax.dot_general(a, b, (((1,), (0,)), ((), ())), preferred_element_type=f32)


def attend_kernel(
    heads, run, pieces, scaling, active, q_in, g_in, *refs
):
    kv_in = refs[:pieces]
    cos, sin, pos_q, first_q, pos_k = refs[pieces : pieces + 5]
    dq_out, dkv_out = refs[pieces + 5 : pieces + 7]
    q_s, k_s, kt_s, v_s, s_s, d_s, dq_s, dk_s, dv_s = refs[pieces + 7 :]
    rows = q_in.shape[0]
    runs = rows // run
    blocks = k_s.shape[0] // run

    for h in range(heads):
        v = q_in[:, h * HEAD : (h + 1) * HEAD]
        q_s[h] = (v * cos[:rows, :] + pltpu.roll(v, HEAD // 2, 1) * sin[:rows, :]).astype(bf16)
    for j in range(pieces):
        at = pl.ds(j * rows, rows)
        v = kv_in[j][:, :HEAD].astype(f32)
        turned = v * cos[at, :] + pltpu.roll(v, HEAD // 2, 1) * sin[at, :]
        k_s[at, :] = turned.astype(bf16)
        kt_s[:, at] = turned.T.astype(bf16)
        v_s[at, :] = kv_in[j][:, HEAD:]
    dk_s[...] = jnp.zeros_like(dk_s)
    dv_s[...] = jnp.zeros_like(dv_s)

    for i in range(runs):
        mine = pl.ds(i * run, run)
        dq_s[...] = jnp.zeros_like(dq_s)
        p_q, f_q = pos_q[:, i * run : (i + 1) * run], first_q[:, i * run : (i + 1) * run]

        def each(body, init):
            def step(kb, carry):
                return lax.cond(
                    active[i * blocks + kb] > 0, functools.partial(body, kb), lambda c: c, carry
                )

            return lax.fori_loop(0, blocks, step, init)

        def fold(x, op):
            x = x.reshape(run // 8, 8, run)
            return op(x, axis=0)

        def peak(kb, carry):
            at = pl.ds(pl.multiple_of(kb * run, run), run)
            p_k = pos_k[at, :]
            seen = (p_k <= p_q) & (p_k >= f_q)
            out = []
            for h in range(heads):
                s = jnp.where(seen, nt(k_s[at, :], q_s[h, mine, :]) * scaling, -1e30)
                s_s[h, at, :] = s
                out.append(jnp.maximum(carry[h], fold(s, jnp.max)))
            return tuple(out)

        top = each(peak, tuple(jnp.full((8, run), -1e30, f32) for _ in range(heads)))
        top = [jnp.max(t, axis=0, keepdims=True) for t in top]

        def expo(kb, carry):
            at = pl.ds(pl.multiple_of(kb * run, run), run)
            out = []
            for h in range(heads):
                e = jnp.exp(s_s[h, at, :] - top[h])
                s_s[h, at, :] = e
                out.append(carry[h] + fold(e, jnp.sum))
            return tuple(out)

        norm = each(expo, tuple(jnp.zeros((8, run), f32) for _ in range(heads)))
        norm = [1.0 / jnp.sum(t, axis=0, keepdims=True) for t in norm]

        def probs(kb, carry):
            at = pl.ds(pl.multiple_of(kb * run, run), run)
            out = []
            total = dv_s[at, :]
            for h in range(heads):
                g = g_in[mine, h * HEAD : (h + 1) * HEAD]
                p = s_s[h, at, :] * norm[h]
                half = p.astype(bf16)
                d = nt(v_s[at, :], g)
                s_s[h, at, :] = p
                d_s[h, at, :] = d
                out.append(carry[h] + fold(half.astype(f32) * d, jnp.sum))
                total = total + nn(half, g)
            dv_s[at, :] = total
            return tuple(out)

        delta = each(probs, tuple(jnp.zeros((8, run), f32) for _ in range(heads)))
        delta = [jnp.sum(t, axis=0, keepdims=True) for t in delta]

        def grads(kb, carry):
            at = pl.ds(pl.multiple_of(kb * run, run), run)
            total = dk_s[at, :]
            for h in range(heads):
                ds = (s_s[h, at, :] * (d_s[h, at, :] - delta[h])).astype(bf16)
                total = total + nn(ds, q_s[h, mine, :])
                dq_s[h] += nn(kt_s[:, at], ds)
            dk_s[at, :] = total
            return carry

        each(grads, 0)
        for h in range(heads):
            d = dq_s[h].T * scaling
            back = d * cos[mine, :] - pltpu.roll(d, HEAD // 2, 1) * sin[mine, :]
            dq_out[mine, h * HEAD : (h + 1) * HEAD] = back.astype(bf16)

    for j in range(pieces):
        at = pl.ds(j * rows, rows)
        d = dk_s[at, :] * scaling
        back = d * cos[at, :] - pltpu.roll(d, HEAD // 2, 1) * sin[at, :]
        dkv_out[at, :HEAD] = back.astype(bf16)
        dkv_out[at, HEAD:] = dv_s[at, :].astype(bf16)


def attend(active, q_raw, upstream, kv, cos, sin, pos_q, first_q, pos_k, run):
    rows, cols = q_raw.shape
    heads = cols // HEAD
    total = pos_k.shape[0]
    vmem = pl.BlockSpec(memory_space=pltpu.VMEM)
    smem = pl.BlockSpec(memory_space=pltpu.SMEM)
    return pl.pallas_call(
        functools.partial(attend_kernel, heads, run, len(kv), HEAD**-0.5),
        out_shape=(
            jax.ShapeDtypeStruct((rows, cols), bf16),
            jax.ShapeDtypeStruct((total, 2 * HEAD), bf16),
        ),
        in_specs=[smem] + [vmem] * (7 + len(kv)),
        out_specs=(vmem, vmem),
        scratch_shapes=[
            pltpu.VMEM((heads, rows, HEAD), bf16),
            pltpu.VMEM((total, HEAD), bf16),
            pltpu.VMEM((HEAD, total), bf16),
            pltpu.VMEM((total, HEAD), bf16),
            pltpu.VMEM((heads, total, run), f32),
            pltpu.VMEM((heads, total, run), f32),
            pltpu.VMEM((heads, HEAD, run), f32),
            pltpu.VMEM((total, HEAD), f32),
            pltpu.VMEM((total, HEAD), f32),
        ],
        compiler_params=pltpu.CompilerParams(vmem_limit_bytes=52 * 2**20),
        name="attend",
    )(active, q_raw, upstream, *kv, cos, sin, pos_q, first_q, pos_k)


def shards(tokens, upstream, w_query, w_keyval, positions, documents):
    ctx, tp = lax.axis_index("ctx"), lax.axis_index("tp")
    ctx_count, tp_count = lax.axis_size("ctx"), lax.axis_size("tp")
    pairs, z, core = tp_count // 2, tp // 2, tp % 2
    own_rows, features = tokens.shape
    rows = own_rows * tp_count
    query_cols, keyval_cols = w_query.shape[1], w_keyval.shape[1]
    weight_rows = w_query.shape[0]
    half = weight_rows // 2
    sharing = (tp_count // KEY_VALUE_HEADS).bit_length() - 1
    bits = [1 << b for b in range(ctx_count.bit_length() - 1)]
    ranks = range(ctx_count)

    weight = jnp.concatenate([w_query, w_keyval], axis=1)
    lower = gather_ctx(weight[:half], bits)
    upper = gather_ctx(weight[half:], bits[::-1])

    part = own_rows // 2
    stacks = [
        gather_line(tokens[:part], pairs, z),
        gather_line(tokens[part:], pairs, z),
    ]
    stack = jnp.concatenate(stacks, axis=1)
    other = swap(stack, "tp", 1)
    gathered = jnp.where(
        core == 0,
        jnp.stack([stack, other], axis=1),
        jnp.stack([other, stack], axis=1),
    ).reshape(rows, features)

    pos = jnp.concatenate(
        [lax.dynamic_slice_in_dim(positions, (ctx ^ j) * rows, rows, 0) for j in ranks]
    )
    seq = pos.shape[0]
    frequency = ROPE_BASE ** (-(jnp.arange(HEAD // 2, dtype=f32) * 2.0 / HEAD))
    angles = pos.astype(f32)[:, None] * frequency[None, :]
    cosine, sine = jnp.cos(angles), jnp.sin(angles)
    cos = jnp.concatenate([cosine, cosine], axis=1)
    sin = jnp.concatenate([-sine, sine], axis=1)
    my_pos = pos[:rows]
    my_doc = jnp.take(documents, my_pos)
    first = jnp.sum((documents[None, :] < my_doc[:, None]).astype(jnp.int32), axis=1)
    run = rows // 2
    low_k, high_k = jnp.min(pos.reshape(-1, run), axis=1), jnp.max(pos.reshape(-1, run), axis=1)
    high_q, low_f = jnp.max(my_pos.reshape(-1, run), axis=1), jnp.min(first.reshape(-1, run), axis=1)
    active = (
        ((low_k[None, :] <= high_q[:, None]) & (high_k[None, :] >= low_f[:, None]))
        .astype(jnp.int32)
        .reshape(-1)
    )

    def columns(j, side):
        return lax.dynamic_slice_in_dim(gathered, (ctx ^ j) * weight_rows + side * half, half, 1)

    raw = jnp.zeros((rows, query_cols + keyval_cols), f32)
    for j in ranks:
        raw = raw + nn(columns(j, 0), lower[j]) + nn(columns(j, 1), upper[j])
    q_raw = raw[:, :query_cols]
    head_kv = raw[:, query_cols:].astype(bf16)
    for bit in range(sharing):
        partner = swap(head_kv, "tp", 1 << bit)
        head_kv = jnp.where(
            tp // (1 << bit) % 2 == 0,
            jnp.concatenate([head_kv, partner], axis=1),
            jnp.concatenate([partner, head_kv], axis=1),
        )
    kv = [head_kv] + [swap(head_kv, "ctx", j) for j in ranks[1:]]
    query_back, kv_terms = attend(
        active, q_raw, upstream, kv, cos, sin, my_pos[None, :], first[None, :], pos[:, None], run
    )

    head_grad = kv_terms[:rows].astype(f32)
    for j in ranks[1:]:
        head_grad = head_grad + swap(kv_terms[j * rows : (j + 1) * rows], "ctx", j).astype(f32)
    for bit in reversed(range(sharing)):
        width = head_grad.shape[1] // 2
        is_lower = tp // (1 << bit) % 2 == 0
        kept = jnp.where(is_lower, head_grad[:, :width], head_grad[:, width:])
        sent = jnp.where(is_lower, head_grad[:, width:], head_grad[:, :width])
        head_grad = kept + swap(sent.astype(bf16), "tp", 1 << bit).astype(f32)
    keyval_back = head_grad.astype(bf16)
    row_grads = jnp.concatenate([query_back, keyval_back], axis=1)

    sums = []
    for held in (lower, upper):
        term = jnp.concatenate([nt(row_grads, held[j]) for j in ranks], axis=1)
        term = term.reshape(pairs, 2, own_rows, -1)
        mine = lax.dynamic_index_in_dim(term, core, 1, keepdims=False)
        theirs = lax.dynamic_index_in_dim(term, 1 - core, 1, keepdims=False).astype(bf16)
        term = mine + swap(theirs, "tp", 1).astype(f32)
        sums.append(scatter_line(term, pairs, z).astype(bf16).reshape(own_rows, ctx_count, half))
    relative = jnp.stack(sums, axis=2).reshape(own_rows, ctx_count, weight_rows)
    token_grad = jnp.concatenate(
        [lax.dynamic_index_in_dim(relative, ctx ^ b, 1, keepdims=False) for b in ranks], axis=1
    )

    def weight_term(j, side):
        return lax.dot_general(
            columns(j, side), row_grads, (((0,), (0,)), ((), ())), preferred_element_type=f32
        )

    weight_grad = jnp.concatenate(
        [
            scatter_ctx({j: weight_term(j, 0) for j in ranks}, bits[::-1]),
            scatter_ctx({j: weight_term(j, 1) for j in ranks}, bits),
        ],
        axis=0,
    )
    return (token_grad, weight_grad[:, :query_cols], weight_grad[:, query_cols:])


def solution(mesh):
    return jax.shard_map(
        shards,
        mesh=mesh,
        in_specs=(P(("ctx", "tp"), None), P("ctx", "tp"), P("ctx", "tp"), P("ctx", "tp"), P(), P()),
        out_specs=(P(("ctx", "tp"), None), P("ctx", "tp"), P("ctx", "tp")),
        check_vma=False,
    )
```

```python
import functools

import jax
import jax.numpy as jnp
from jax import lax
from jax.experimental import pallas as pl
from jax.experimental.pallas import tpu as pltpu
from jax.sharding import PartitionSpec as P


KEY_VALUE_HEADS = 8
HEAD = 128
ROPE_BASE = 500000.0


f32 = jnp.float32
bf16 = jnp.bfloat16


def swap(block, axis, mask):
    count = lax.axis_size(axis)
    return lax.ppermute(block, axis, [(i, i ^ mask) for i in range(count)])


def hop(block, step, first, last):
    route = [(2 * z + c, 2 * (z + step) + c) for z in range(first, last + 1) for c in (0, 1)]
    return lax.ppermute(block, "tp", route)


def gather_order(bits):
    held = [0]
    for bit in bits:
        held += [j | bit for j in held]
    return held[1:]


def gather_ctx(block, bits):
    held = {0: block}
    for bit in bits:
        for j in list(held):
            held[j | bit] = swap(held[j], "ctx", bit)
    return held


def scatter_ctx(terms, bits):
    terms = dict(terms)
    for bit in bits:
        for j in sorted((j for j in terms if j & bit), reverse=True):
            got = swap(terms.pop(j).astype(bf16), "ctx", bit)
            terms[j ^ bit] = terms[j ^ bit].astype(f32) + got.astype(f32)
    return terms[0]


def gather_line(block, pairs, z):
    right, left = {0: block}, {0: block}
    for s in range(1, pairs):
        right[s] = hop(right[s - 1], 1, s - 1, pairs - 2)
        left[s] = hop(left[s - 1], -1, 1, pairs - s)
    stack = jnp.zeros((pairs,) + block.shape, block.dtype)
    stack = lax.dynamic_update_index_in_dim(stack, block, z, 0)
    for s in range(1, pairs):
        come = jnp.where(z >= s, right[s], left[pairs - s])
        stack = lax.dynamic_update_index_in_dim(stack, come, (z - s) % pairs, 0)
    return stack


def scatter_line(stack, pairs, z):
    def pick(at):
        return lax.dynamic_index_in_dim(stack, at % pairs, 0, keepdims=False)

    right, left = None, None
    for s in range(1, pairs):
        to_right, to_left = pick(z - s), pick(z + s)
        if right is not None:
            to_right = to_right + right.astype(f32)
            to_left = to_left + left.astype(f32)
        right = hop(to_right.astype(bf16), 1, 0, s - 1)
        left = hop(to_left.astype(bf16), -1, pairs - s, pairs - 1)
    return pick(z) + right.astype(f32) + left.astype(f32)


def nt(a, b):
    return lax.dot_general(a, b, (((1,), (1,)), ((), ())), preferred_element_type=f32)


def nn(a, b):
    return lax.dot_general(a, b, (((1,), (0,)), ((), ())), preferred_element_type=f32)


def attend_kernel(
    heads, run, pieces, scaling, active, q_in, g_in, *refs
):
    kv_in = refs[:pieces]
    cos, sin, pos_q, first_q, pos_k = refs[pieces : pieces + 5]
    dq_out = refs[pieces + 5]
    dkv_out = refs[pieces + 6 : 2 * pieces + 6]
    q_s, k_s, kt_s, v_s, s_s, d_s, dq_s, dk_s, dv_s = refs[2 * pieces + 6 :]
    rows = q_in.shape[0]
    runs = rows // run
    blocks = k_s.shape[0] // run

    for h in range(heads):
        v = q_in[:, h * HEAD : (h + 1) * HEAD]
        q_s[h] = (v * cos[:rows, :] + pltpu.roll(v, HEAD // 2, 1) * sin[:rows, :]).astype(bf16)
    for j in range(pieces):
        at = pl.ds(j * rows, rows)
        v = kv_in[j][:, :HEAD].astype(f32)
        turned = v * cos[at, :] + pltpu.roll(v, HEAD // 2, 1) * sin[at, :]
        k_s[at, :] = turned.astype(bf16)
        kt_s[:, at] = turned.T.astype(bf16)
        v_s[at, :] = kv_in[j][:, HEAD:]
    dk_s[...] = jnp.zeros_like(dk_s)
    dv_s[...] = jnp.zeros_like(dv_s)

    def one_run(i, unused):
        mine = pl.ds(pl.multiple_of(i * run, run), run)
        dq_s[...] = jnp.zeros_like(dq_s)
        p_q, f_q = pos_q[pl.ds(i, 1), :], first_q[pl.ds(i, 1), :]

        def each(body, init):
            def step(kb, carry):
                return lax.cond(
                    active[i * blocks + kb] > 0, functools.partial(body, kb), lambda c: c, carry
                )

            return lax.fori_loop(0, blocks, step, init)

        def fold(x, op):
            x = x.reshape(run // 8, 8, run)
            return op(x, axis=0)

        def peak(kb, carry):
            at = pl.ds(pl.multiple_of(kb * run, run), run)
            p_k = pos_k[at, :1]
            seen = (p_k <= p_q) & (p_k >= f_q)
            out = []
            for h in range(heads):
                s = jnp.where(seen, nt(k_s[at, :], q_s[h, mine, :]) * scaling, -1e30)
                s_s[h, at, :] = s
                out.append(jnp.maximum(carry[h], fold(s, jnp.max)))
            return tuple(out)

        top = each(peak, tuple(jnp.full((8, run), -1e30, f32) for _ in range(heads)))
        top = [jnp.max(t, axis=0, keepdims=True) for t in top]

        def expo(kb, carry):
            at = pl.ds(pl.multiple_of(kb * run, run), run)
            out = []
            for h in range(heads):
                e = jnp.exp(s_s[h, at, :] - top[h])
                s_s[h, at, :] = e
                out.append(carry[h] + fold(e, jnp.sum))
            return tuple(out)

        norm = each(expo, tuple(jnp.zeros((8, run), f32) for _ in range(heads)))
        norm = [1.0 / jnp.sum(t, axis=0, keepdims=True) for t in norm]

        def probs(kb, carry):
            at = pl.ds(pl.multiple_of(kb * run, run), run)
            out = []
            total = dv_s[at, :]
            for h in range(heads):
                g = g_in[mine, h * HEAD : (h + 1) * HEAD]
                p = s_s[h, at, :] * norm[h]
                half = p.astype(bf16)
                d = nt(v_s[at, :], g)
                s_s[h, at, :] = p
                d_s[h, at, :] = d
                out.append(carry[h] + fold(half.astype(f32) * d, jnp.sum))
                total = total + nn(half, g)
            dv_s[at, :] = total
            return tuple(out)

        delta = each(probs, tuple(jnp.zeros((8, run), f32) for _ in range(heads)))
        delta = [jnp.sum(t, axis=0, keepdims=True) for t in delta]

        def grads(kb, carry):
            at = pl.ds(pl.multiple_of(kb * run, run), run)
            total = dk_s[at, :]
            for h in range(heads):
                ds = (s_s[h, at, :] * (d_s[h, at, :] - delta[h])).astype(bf16)
                total = total + nn(ds, q_s[h, mine, :])
                dq_s[h] += nn(kt_s[:, at], ds)
            dk_s[at, :] = total
            return carry

        each(grads, 0)
        for h in range(heads):
            d = dq_s[h].T * scaling
            back = d * cos[mine, :] - pltpu.roll(d, HEAD // 2, 1) * sin[mine, :]
            dq_out[mine, h * HEAD : (h + 1) * HEAD] = back.astype(bf16)
        return unused

    lax.fori_loop(0, runs, one_run, 0)

    for j in range(pieces):
        at = pl.ds(j * rows, rows)
        d = dk_s[at, :] * scaling
        back = d * cos[at, :] - pltpu.roll(d, HEAD // 2, 1) * sin[at, :]
        dkv_out[j][:, :HEAD] = back.astype(bf16)
        dkv_out[j][:, HEAD:] = dv_s[at, :].astype(bf16)


def attend(active, raw, upstream, kv, cos, sin, pos_q, first_q, pos_k, run):
    rows, cols = upstream.shape
    heads = cols // HEAD
    total = pos_k.shape[0]
    vmem = pl.BlockSpec(memory_space=pltpu.VMEM)
    smem = pl.BlockSpec(memory_space=pltpu.SMEM)
    return pl.pallas_call(
        functools.partial(attend_kernel, heads, run, len(kv), HEAD**-0.5),
        out_shape=[jax.ShapeDtypeStruct((rows, cols), bf16)]
        + [jax.ShapeDtypeStruct((rows, 2 * HEAD), bf16)] * len(kv),
        in_specs=[smem] + [vmem] * (7 + len(kv)),
        out_specs=[vmem] * (1 + len(kv)),
        scratch_shapes=[
            pltpu.VMEM((heads, rows, HEAD), bf16),
            pltpu.VMEM((total, HEAD), bf16),
            pltpu.VMEM((HEAD, total), bf16),
            pltpu.VMEM((total, HEAD), bf16),
            pltpu.VMEM((heads, total, run), f32),
            pltpu.VMEM((heads, total, run), f32),
            pltpu.VMEM((heads, HEAD, run), f32),
            pltpu.VMEM((total, HEAD), f32),
            pltpu.VMEM((total, HEAD), f32),
        ],
        compiler_params=pltpu.CompilerParams(vmem_limit_bytes=52 * 2**20),
        name="attend",
    )(active, raw, upstream, *kv, cos, sin, pos_q, first_q, pos_k)


def shards(tokens, upstream, w_query, w_keyval, positions, documents):
    ctx, tp = lax.axis_index("ctx"), lax.axis_index("tp")
    ctx_count, tp_count = lax.axis_size("ctx"), lax.axis_size("tp")
    pairs, z, core = tp_count // 2, tp // 2, tp % 2
    own_rows, features = tokens.shape
    rows = own_rows * tp_count
    query_cols, keyval_cols = w_query.shape[1], w_keyval.shape[1]
    weight_rows = w_query.shape[0]
    half = weight_rows // 2
    sharing = (tp_count // KEY_VALUE_HEADS).bit_length() - 1
    bits = [1 << b for b in range(ctx_count.bit_length() - 1)]
    ranks = range(ctx_count)

    weight = jnp.concatenate([w_query, w_keyval], axis=1)
    lower = gather_ctx(weight[:half], bits)
    upper = gather_ctx(weight[half:], bits[::-1])

    pos = jnp.concatenate(
        [lax.dynamic_slice_in_dim(positions, (ctx ^ j) * rows, rows, 0) for j in ranks]
    )
    frequency = ROPE_BASE ** (-(jnp.arange(HEAD // 2, dtype=f32) * 2.0 / HEAD))
    angles = pos.astype(f32)[:, None] * jnp.concatenate([frequency, frequency])[None, :]
    cos = jnp.cos(angles)
    sin = jnp.sin(angles) * jnp.where(jnp.arange(HEAD) < HEAD // 2, -1.0, 1.0)[None, :]
    pos_k = jnp.broadcast_to(pos[:, None], (pos.shape[0], HEAD))
    my_pos = pos[:rows]
    my_doc = jnp.take(documents, my_pos)
    first = jnp.sum((documents[None, :] < my_doc[:, None]).astype(jnp.int32), axis=1)
    run = rows // 2
    by_run = pos.reshape(-1, run)
    pos_q, first_q = my_pos.reshape(-1, run), first.reshape(-1, run)
    low_k, high_k = jnp.min(by_run, axis=1), jnp.max(by_run, axis=1)
    high_q, low_f = jnp.max(pos_q, axis=1), jnp.min(first_q, axis=1)
    active = (
        ((low_k[None, :] <= high_q[:, None]) & (high_k[None, :] >= low_f[:, None]))
        .astype(jnp.int32)
        .reshape(-1)
    )

    part = own_rows // 2
    stacks = [gather_line(tokens[:part], pairs, z), gather_line(tokens[part:], pairs, z)]
    stack = jnp.concatenate(stacks, axis=1)
    stack, cos, sin, pos_k, pos_q, first_q, active = lax.optimization_barrier(
        (stack, cos, sin, pos_k, pos_q, first_q, active)
    )
    other = swap(stack, "tp", 1)
    gathered = jnp.where(
        core == 0,
        jnp.stack([stack, other], axis=1),
        jnp.stack([other, stack], axis=1),
    ).reshape(rows, features)
    turned = gathered.T

    def columns(j, side):
        return lax.dynamic_slice_in_dim(gathered, (ctx ^ j) * weight_rows + side * half, half, 1)

    steps = [(0, 0), (0, 1)]
    for a, b in zip(gather_order(bits), gather_order(bits[::-1])):
        steps += [(a, 0), (b, 1)]
    raw = jnp.zeros((rows, query_cols + keyval_cols), f32)
    for at, (j, side) in enumerate(steps):
        if at == len(steps) - 2:
            raw, turned = lax.optimization_barrier((raw, turned))
        raw = raw + nn(columns(j, side), (lower, upper)[side][j])
    head_kv = raw[:, query_cols:].astype(bf16)
    lower, upper, head_kv = lax.optimization_barrier((lower, upper, head_kv))
    for bit in range(sharing):
        partner = swap(head_kv, "tp", 1 << bit)
        head_kv = jnp.where(
            tp // (1 << bit) % 2 == 0,
            jnp.concatenate([head_kv, partner], axis=1),
            jnp.concatenate([partner, head_kv], axis=1),
        )
    kv = [head_kv] + [swap(head_kv, "ctx", j) for j in ranks[1:]]
    lower_all = jnp.concatenate([lower[j] for j in ranks], axis=0)
    upper_all = jnp.concatenate([upper[j] for j in ranks], axis=0)
    kv, lower_all, upper_all = lax.optimization_barrier((kv, lower_all, upper_all))
    query_back, *kv_terms = attend(
        active, raw, upstream, kv, cos, sin, pos_q, first_q, pos_k, run
    )

    head_grad = kv_terms[0].astype(f32)
    for j in ranks[:0:-1]:
        head_grad = head_grad + swap(kv_terms[j], "ctx", j).astype(f32)
    for bit in reversed(range(sharing)):
        width = head_grad.shape[1] // 2
        is_lower = tp // (1 << bit) % 2 == 0
        kept = jnp.where(is_lower, head_grad[:, :width], head_grad[:, width:])
        sent = jnp.where(is_lower, head_grad[:, width:], head_grad[:, :width])
        head_grad = kept + swap(sent.astype(bf16), "tp", 1 << bit).astype(f32)
    row_grads = jnp.concatenate([query_back, head_grad.astype(bf16)], axis=1)

    by_core = row_grads.reshape(pairs, 2, own_rows, -1)
    mine = lax.dynamic_index_in_dim(by_core, core, 1, keepdims=False).reshape(rows // 2, -1)
    theirs = lax.dynamic_index_in_dim(by_core, 1 - core, 1, keepdims=False).reshape(rows // 2, -1)
    sums = []
    for held in (lower_all, upper_all):
        got = swap(nt(theirs, held).astype(bf16), "tp", 1)
        term = (nt(mine, held) + got.astype(f32)).reshape(pairs, own_rows, -1)
        done = scatter_line(term, pairs, z).astype(bf16)
        sums.append(done.reshape(own_rows, ctx_count, half))
    relative = jnp.stack(sums, axis=2).reshape(own_rows, ctx_count, weight_rows)
    token_grad = jnp.concatenate(
        [lax.dynamic_index_in_dim(relative, ctx ^ b, 1, keepdims=False) for b in ranks], axis=1
    )

    def weight_term(j, side):
        at = (ctx ^ j) * weight_rows + side * half
        return nn(lax.dynamic_slice_in_dim(turned, at, half, 0), row_grads).astype(bf16)

    weight_grad = jnp.concatenate(
        [
            scatter_ctx({j: weight_term(j, 0) for j in ranks}, bits[::-1]),
            scatter_ctx({j: weight_term(j, 1) for j in ranks}, bits),
        ],
        axis=0,
    )
    return (token_grad, weight_grad[:, :query_cols], weight_grad[:, query_cols:])


def solution(mesh):
    return jax.shard_map(
        shards,
        mesh=mesh,
        in_specs=(P(("ctx", "tp"), None), P("ctx", "tp"), P("ctx", "tp"), P("ctx", "tp"), P(), P()),
        out_specs=(P(("ctx", "tp"), None), P("ctx", "tp"), P("ctx", "tp")),
        check_vma=False,
    )
```
